32 devices in a mesh: groups: 2 (over y), blk: 16 (over z, x, core).
Axes of the slice: x: 2, y: 2, z: 4, core: 2. Of those that a mesh axis runs over, the one named last changes fastest.
Arguments:
- current_states: float32 [16, 8192], P(None, ('groups', 'blk')), parts along dimension 1, may hold values from -0.5 to 0.5
- next_states: float32 [16, 8192], P(None, ('groups', 'blk')), parts along dimension 1, may hold values from -1 to 1
- next_values: float32 [8192], P(('groups', 'blk')), parts along dimension 0, may hold values from 0 to 2.5
- vol_table: float32 [12, 16], replicated, may hold values from 0.15 to 0.45
- date_index: int32 [1], replicated, may hold values from 0 to 11
- strike: float32 [1], replicated, may hold values from 0.8 to 1.2
Outputs:
- continuation: float32 [8192], P(('groups', 'blk')), parts along dimension 0
- node_value: float32 [8192], P(('groups', 'blk')), parts along dimension 0
The draws below stay inside these ranges and needn't reach their ends.
There are 2 independent parts, one for each index of `groups`. The reference program is written for one: setup_inputs(seed, part) draws one part's arguments, and reference() takes and returns one part's arrays. A program takes and returns all parts, laid end to end along the dimension named above; an argument that names none is the same for every part. Nothing has to cross between parts.
All inputs are finite; a program needn't handle non-finite values.
Results may differ from the reference program's by a relative error of at most 0.00012.
Values sent between devices are 32-bit elements; how exact they have to be, the bound alone decides.
A program may use at most 64 MiB of HBM per device.

```python
import math
import jax
import jax.numpy as jnp
from jax import lax

ASSETS = 16
DATES = 12
NODES = 4096


def mesh_paths(key):
    folded = jax.random.fold_in(key, 7)
    key_list = jax.random.split(folded, 5)
    placing = (jnp.arange(NODES, dtype=jnp.float32) + 0.5) / NODES - 0.5
    heading = 0.05 * jnp.clip(jax.random.normal(key_list[0], (ASSETS,), jnp.float32), -2.0, 2.0)
    widths = jnp.exp(jax.random.uniform(key_list[1], (ASSETS,), jnp.float32, jnp.log(0.5), jnp.log(1.5)))
    jitter = jnp.clip(jax.random.normal(key_list[2], (ASSETS, NODES), jnp.float32), -4.0, 4.0)
    current = 0.03 * widths[:, None] * jitter + heading[:, None] * placing[None, :]
    moves = jnp.clip(jax.random.normal(key_list[3], (ASSETS, NODES), jnp.float32), -4.0, 4.0)
    following = current - 0.004 + 0.095 * moves
    extra = jnp.clip(jax.random.normal(key_list[4], (NODES,), jnp.float32), -4.0, 4.0)
    worth = jnp.maximum(jnp.max(jnp.exp(following), axis=0) - 1.0, 0.0) + 0.05 * jnp.exp(0.5 * extra)
    return (current, following, worth)


def draw_current_states(key, part):
    return mesh_paths(key)[0]


def draw_next_states(key, part):
    return mesh_paths(key)[1]


def draw_next_values(key, part):
    return mesh_paths(key)[2]


def setup_inputs(seed: int = 0, part: int = 0) -> dict:
    keys = jax.random.split(jax.random.key(seed), 7)
    own_keys = jax.random.split(jax.random.fold_in(keys[6], part), 7)
    return {
        "current_states": draw_current_states(jax.random.fold_in(jax.random.fold_in(keys[6], part), 71), part),
        "next_states": draw_next_states(jax.random.fold_in(jax.random.fold_in(keys[6], part), 71), part),
        "next_values": draw_next_values(jax.random.fold_in(jax.random.fold_in(keys[6], part), 71), part),
        "vol_table": jnp.clip(jnp.exp(jax.random.uniform(keys[3], (DATES, ASSETS), jnp.float32, math.log(0.15), math.log(0.45))), 0.15, 0.45),
        "date_index": jax.random.randint(keys[4], (1,), 0, DATES).astype(jnp.int32),
        "strike": jnp.clip(jax.random.uniform(keys[5], (1,), jnp.float32, 0.8, 1.2), 0.8, 1.2),
    }


rate_year = 0.05
step_years = 0.1

def scaled_states(current_states, next_states, vol_table, date_index):
    date_count = vol_table.shape[0]
    picked = (jnp.arange(date_count, dtype=jnp.int32) == date_index[0]).astype(jnp.float32)
    vol_row = lax.optimization_barrier(jnp.sum(vol_table * picked[:, None], axis=0))
    spread = vol_row * math.sqrt(step_years)
    drift_term = (rate_year - 0.5 * vol_row * vol_row) * step_years
    anchor = (current_states + drift_term[:, None]) / spread[:, None]
    target = next_states / spread[:, None]
    anchor_half = 0.5 * lax.optimization_barrier(jnp.sum(anchor * anchor, axis=0, keepdims=True))
    target_half = 0.5 * lax.optimization_barrier(jnp.sum(target * target, axis=0, keepdims=True))
    return (anchor, anchor_half, target, target_half)

def kernel_block(source_states, source_norms, sink_states, sink_norms):
    inner_term = lax.dot_general(source_states, sink_states, (((0,), (0,)), ((), ())), precision=lax.Precision.HIGHEST, preferred_element_type=jnp.float32)
    return jnp.exp(inner_term - source_norms.reshape(-1, 1) - sink_norms.reshape(1, -1))

def finish(current_states, totals, strike):
    continuation = math.exp(-rate_year * step_years) * totals[0] / totals[1]
    payoff = jnp.maximum(lax.optimization_barrier(jnp.max(jnp.exp(current_states), axis=0)) - strike[0], 0.0)
    return (continuation, jnp.maximum(payoff, continuation))

def reference(current_states, next_states, next_values, vol_table, date_index, strike):
    anchor, anchor_half, target, target_half = scaled_states(current_states, next_states, vol_table, date_index)
    node_count = anchor.shape[1]
    block_size = math.gcd(node_count, 1024)
    blocks = node_count // block_size

    def density_block(number):
        sink_part = lax.dynamic_slice_in_dim(target, number * block_size, block_size, 1)
        norm_part = lax.dynamic_slice_in_dim(target_half, number * block_size, block_size, 1)
        return lax.optimization_barrier(jnp.sum(kernel_block(sink_part, norm_part, anchor, anchor_half), axis=1))
    density = lax.map(density_block, jnp.arange(blocks, dtype=jnp.int32)).reshape(-1)
    ratios = jnp.stack([next_values / density, 1.0 / density], axis=0)

    def weighted_block(number):
        anchor_part = lax.dynamic_slice_in_dim(anchor, number * block_size, block_size, 1)
        half_part = lax.dynamic_slice_in_dim(anchor_half, number * block_size, block_size, 1)
        weights = kernel_block(target, target_half, anchor_part, half_part)
        return jnp.dot(ratios, weights, precision=lax.Precision.HIGHEST, preferred_element_type=jnp.float32)
    totals = lax.map(weighted_block, jnp.arange(blocks, dtype=jnp.int32))
    totals = jnp.transpose(totals, (1, 0, 2)).reshape(2, -1)
    return finish(current_states, totals, strike)
```

```python
import functools
import math

import jax
import jax.numpy as jnp
from jax import lax
from jax.experimental import pallas as pl
from jax.experimental.pallas import tpu as pltpu
from jax.sharding import PartitionSpec as P

rate_year = 0.05
step_years = 0.1
MESH = pl.DeviceIdType.MESH


def grid_masks(count):
    digits = count.bit_length() - 1
    assert 2**digits == count
    inner_digits = digits // 2
    inner_units = ([1] + [1 << (digits - k) for k in range(1, inner_digits)])[:inner_digits]
    outer_units = [1 << k for k in range(digits) if 1 << k not in inner_units]
    if inner_units and outer_units:
        outer_units[-1] |= 1

    def span(units):
        masks = [0]
        for unit in units:
            masks += [mask ^ unit for mask in masks]
        return masks

    return span(inner_units), span(outer_units)


def split3(x):
    high = x.astype(jnp.bfloat16)
    rest = x - high.astype(jnp.float32)
    mid = rest.astype(jnp.bfloat16)
    low = (rest - mid.astype(jnp.float32)).astype(jnp.bfloat16)
    return high, mid, low


def norm_rows(x, first):
    norm = -0.5 * jnp.sum(x * x, axis=0, keepdims=True)
    pieces = [piece.astype(jnp.float32) for piece in split3(norm)]
    row = lax.broadcasted_iota(jnp.int32, (16, x.shape[1]), 0)
    at = 0 if first else 3
    rows = jnp.where((row >= 3 - at) & (row < 6 - at), 1.0, 0.0)
    for number, piece in enumerate(pieces):
        rows = jnp.where(row == at + number, piece, rows)
    return rows.astype(jnp.bfloat16)


def anchor_stack(x):
    high, mid, low = split3(x)
    zero = jnp.zeros_like(high)
    return jnp.concatenate([high, high, high, mid, mid, low, norm_rows(x, True), zero], axis=0)


def target_stack(x):
    high, mid, low = split3(x)
    zero = jnp.zeros_like(high)
    return jnp.concatenate([high, mid, low, high, mid, high, norm_rows(x, False), zero], axis=0)


def kernel(
    inner,
    outer,
    cur_hbm,
    next_hbm,
    val_hbm,
    vol_hbm,
    date_hbm,
    weighted_ref,
    mass_ref,
    best_ref,
    anc,
    tgt,
    val,
    vol,
    date,
    rows,
    columns,
    kmat,
    dens_own,
    dens_in,
    part_own,
    part_in,
    in_sem,
    send_sem,
    tgt_recv,
    anc_recv,
    val_recv,
    dens_recv,
    part_recv,
):
    g, h = len(inner), len(outer)
    n = anc.shape[2]
    near = min(g, 2)
    me = lax.axis_index("blk")

    loads = [
        pltpu.make_async_copy(src, dst, in_sem.at[number])
        for number, (src, dst) in enumerate(
            [
                (next_hbm, tgt.at[0]),
                (cur_hbm, anc.at[0]),
                (vol_hbm, vol),
                (date_hbm, date),
                (val_hbm, val.at[0]),
            ]
        )
    ]
    for load in loads:
        load.start()

    barrier = pltpu.get_barrier_semaphore()
    far_first = list(range(g - 1, 0, -1)), list(range(h - 1, 0, -1))
    for masks, offsets in zip((inner, outer), far_first):
        for offset in offsets:
            pl.semaphore_signal(barrier, inc=1, device_id={"blk": me ^ masks[offset]}, device_id_type=MESH)

    def copy(src, dst, send, recv, mask):
        return pltpu.make_async_remote_copy(
            src_ref=src,
            dst_ref=dst,
            send_sem=send,
            recv_sem=recv,
            device_id={"blk": me ^ mask},
            device_id_type=MESH,
        )

    def tgt_sem(q):
        return tgt_recv.at[0 if q < near else 1]

    tgt_copies = {q: copy(tgt.at[0], tgt.at[q], send_sem.at[0], tgt_sem(q), inner[q]) for q in far_first[0]}
    anc_copies = {s: copy(anc.at[0], anc.at[s], send_sem.at[1], anc_recv, outer[s]) for s in far_first[1]}
    val_copies = {q: copy(val.at[0], val.at[q], send_sem.at[2], val_recv, inner[q]) for q in far_first[0]}
    dens_copies = {q: copy(dens_own, dens_in.at[q], send_sem.at[3], dens_recv, inner[q]) for q in far_first[0]}
    part_copies = {s: copy(part_own.at[s], part_in.at[s], send_sem.at[4], part_recv, outer[s]) for s in far_first[1]}

    def several(ref, first, last, send, recv):
        span = ref.at[pl.ds(first, last - first)]
        return copy(span, span, send, recv, 1)

    pl.semaphore_wait(barrier, (h - 1) + (g - 1))
    loads[0].wait()
    for each in tgt_copies.values():
        each.start()
    loads[1].wait()
    for each in anc_copies.values():
        each.start()
    for load in loads[2:]:
        load.wait()
    for each in val_copies.values():
        each.start()

    dates, assets = vol.shape
    picked = lax.broadcasted_iota(jnp.int32, (dates, assets), 0) == date[0]
    vol_lanes = jnp.sum(jnp.where(picked, vol[...], 0.0), axis=0, keepdims=True)
    eye = lax.broadcasted_iota(jnp.int32, (assets, assets), 0) == lax.broadcasted_iota(
        jnp.int32, (assets, assets), 1
    )
    vol_row = jnp.sum(jnp.where(eye, vol_lanes, 0.0), axis=1, keepdims=True)
    scale = math.sqrt(math.log2(math.e)) / (vol_row * math.sqrt(step_years))
    drift = (rate_year - 0.5 * vol_row * vol_row) * step_years

    def take_anchor(s):
        rows[s] = jnp.transpose(anchor_stack((anc[s] + drift) * scale))

    def take_target(q):
        columns[q] = target_stack(tgt[q] * scale)

    def block(s, q):
        exponent = jnp.dot(rows[s], columns[q], preferred_element_type=jnp.float32)
        weights = jnp.exp2(exponent)
        kmat[s, :, q * n : (q + 1) * n] = weights
        return jnp.sum(weights.reshape(n // 8, 8, n), axis=0)

    density = {}
    take_anchor(0)
    take_target(0)
    density[0] = block(0, 0)
    if near > 1:
        several(tgt, 1, 2, send_sem.at[0], tgt_recv.at[0]).wait_recv()
        take_target(1)
        density[1] = block(0, 1)
    if h > 1:
        several(anc, 1, h, send_sem.at[1], anc_recv).wait_recv()
        for s in range(1, h):
            take_anchor(s)
        for s in range(1, h):
            for q in range(near):
                density[q] = density[q] + block(s, q)
    for q in range(near):
        dens_own[q] = jnp.sum(density[q], axis=0, keepdims=True)
    if g > near:
        several(tgt, near, g, send_sem.at[0], tgt_recv.at[1]).wait_recv()
        for q in range(near, g):
            take_target(q)
        for q in range(near, g):
            density[q] = jnp.zeros((8, n), jnp.float32)
        for s in range(h):
            for q in range(near, g):
                density[q] = density[q] + block(s, q)
        for q in range(near, g):
            dens_own[q] = jnp.sum(density[q], axis=0, keepdims=True)

    for each in dens_copies.values():
        each.start()
    best = jnp.max(jnp.exp(anc[0]), axis=0, keepdims=True)
    if g > 1:
        several(val, 1, g, send_sem.at[2], val_recv).wait_recv()
        several(dens_in, 1, g, send_sem.at[3], dens_recv).wait_recv()
    worth, inverse = {}, {}
    for q in range(g):
        total = dens_own[q]
        for p in range(1, g):
            total = total + dens_in[p, q ^ p]
        inverse[q] = 1.0 / total
        worth[q] = val[q] / total

    for s in [*far_first[1], 0]:
        for r in range(0, n, 128):
            weighted = jnp.zeros((128, 128), jnp.float32)
            mass = jnp.zeros((128, 128), jnp.float32)
            for q in range(g):
                for c in range(0, n, 128):
                    tile = kmat[s, r : r + 128, q * n + c : q * n + c + 128]
                    weighted = weighted + tile * worth[q][:, c : c + 128]
                    mass = mass + tile * inverse[q][:, c : c + 128]
            part_own[s, 0:1, r : r + 128] = jnp.sum(jnp.transpose(weighted), axis=0, keepdims=True)
            part_own[s, 1:2, r : r + 128] = jnp.sum(jnp.transpose(mass), axis=0, keepdims=True)
        if s:
            part_copies[s].start()
    sums = part_own[0]
    if h > 1:
        several(part_in, 1, h, send_sem.at[4], part_recv).wait_recv()
    for s in range(1, h):
        sums = sums + part_in[s]
    weighted_ref[...] = sums[0]
    mass_ref[...] = sums[1]
    best_ref[...] = best.reshape(n)
    if g > 1:
        several(tgt, 1, g, send_sem.at[0], tgt_recv.at[0]).wait_send()
        several(val, 1, g, send_sem.at[2], val_recv).wait_send()
        several(dens_in, 1, g, send_sem.at[3], dens_recv).wait_send()
    if h > 1:
        several(anc, 1, h, send_sem.at[1], anc_recv).wait_send()
        several(part_in, 1, h, send_sem.at[4], part_recv).wait_send()


def body(count, current_states, next_states, next_values, vol_table, date_index, strike):
    assets, n = current_states.shape
    inner, outer = grid_masks(count)
    g, h = len(inner), len(outer)
    f32, bf16 = jnp.float32, jnp.bfloat16
    dma = pltpu.SemaphoreType.DMA
    row = pltpu.VMEM((n,), f32)
    w, m, p = pl.pallas_call(
        functools.partial(kernel, inner, outer),
        out_shape=(row, row, row),
        in_specs=[pl.BlockSpec(memory_space=pltpu.HBM)] * 5,
        out_specs=(pl.BlockSpec(memory_space=pltpu.VMEM),) * 3,
        scratch_shapes=[
            pltpu.VMEM((h, assets, n), f32),
            pltpu.VMEM((g, assets, n), f32),
            pltpu.VMEM((g, 1, n), f32),
            pltpu.VMEM(vol_table.shape, f32),
            pltpu.SMEM((1,), jnp.int32),
            pltpu.VMEM((h, n, 8 * assets), bf16),
            pltpu.VMEM((g, 8 * assets, n), bf16),
            pltpu.VMEM((h, n, g * n), f32),
            pltpu.VMEM((g, 1, n), f32),
            pltpu.VMEM((g, g, 1, n), f32),
            pltpu.VMEM((h, 2, n), f32),
            pltpu.VMEM((h, 2, n), f32),
            dma((5,)),
            dma((5,)),
            dma((2,)),
            dma,
            dma,
            dma,
            dma,
        ],
        compiler_params=pltpu.CompilerParams(collective_id=0, has_side_effects=True),
    )(current_states, next_states, next_values.reshape(1, n), vol_table, date_index)
    c = math.exp(-rate_year * step_years) * w / m
    return (c, jnp.maximum(jnp.maximum(p - strike[0], 0.0), c))


def solution(mesh):
    placed = (
        P(None, ("groups", "blk")),
        P(None, ("groups", "blk")),
        P(("groups", "blk")),
        P(),
        P(),
        P(),
    )
    return jax.shard_map(
        functools.partial(body, mesh.shape["blk"]),
        mesh=mesh,
        in_specs=placed,
        out_specs=(P(("groups", "blk")), P(("groups", "blk"))),
        check_vma=False,
    )
```

```python
import functools
import math

import jax
import jax.numpy as jnp
from jax import lax
from jax.experimental import pallas as pl
from jax.experimental.pallas import tpu as pltpu
from jax.sharding import PartitionSpec as P

rate_year = 0.05
step_years = 0.1
MESH = pl.DeviceIdType.MESH


def grid_masks(count):
    digits = count.bit_length() - 1
    assert 2**digits == count
    inner_digits = digits // 2
    inner_units = ([1] + [1 << (digits - k) for k in range(1, inner_digits)])[:inner_digits]
    outer_units = [1 << k for k in range(digits) if 1 << k not in inner_units]
    if inner_units and outer_units:
        outer_units[-1] |= 1

    def span(units):
        masks = [0]
        for unit in units:
            masks += [mask ^ unit for mask in masks]
        return masks

    return span(inner_units), span(outer_units)


def reader(place, inner):
    digits = functools.reduce(lambda a, b: a | b, inner)
    return (place & digits) == (digits & 1)


def split3(x):
    high = x.astype(jnp.bfloat16)
    rest = x - high.astype(jnp.float32)
    mid = rest.astype(jnp.bfloat16)
    low = (rest - mid.astype(jnp.float32)).astype(jnp.bfloat16)
    return high, mid, low


def norm_rows(x, first):
    norm = -0.5 * jnp.sum(x * x, axis=0, keepdims=True)
    pieces = [piece.astype(jnp.float32) for piece in split3(norm)]
    row = lax.broadcasted_iota(jnp.int32, (16, x.shape[1]), 0)
    at = 0 if first else 3
    rows = jnp.where((row >= 3 - at) & (row < 6 - at), 1.0, 0.0)
    for number, piece in enumerate(pieces):
        rows = jnp.where(row == at + number, piece, rows)
    return rows.astype(jnp.bfloat16)


def anchor_stack(x):
    high, mid, low = split3(x)
    zero = jnp.zeros_like(high)
    return jnp.concatenate([high, high, high, mid, mid, low, norm_rows(x, True), zero], axis=0)


def target_stack(x):
    high, mid, low = split3(x)
    zero = jnp.zeros_like(high)
    return jnp.concatenate([high, mid, low, high, mid, high, norm_rows(x, False), zero], axis=0)


def kernel(
    inner,
    outer,
    cur_hbm,
    next_hbm,
    val_hbm,
    vol_hbm,
    facts_ref,
    weighted_ref,
    mass_ref,
    payoff_ref,
    anc,
    tgt,
    val,
    vol,
    facts,
    rows,
    columns,
    kmat,
    dens_own,
    dens_in,
    part_own,
    part_in,
    in_sem,
    send_sem,
    tgt_recv,
    anc_recv,
    val_recv,
    facts_recv,
    dens_recv,
    part_recv,
):
    g, h = len(inner), len(outer)
    n = anc.shape[2]
    near = min(g, 2)
    me = lax.axis_index("blk")

    loads = [
        pltpu.make_async_copy(src, dst, in_sem.at[number])
        for number, (src, dst) in enumerate(
            [
                (next_hbm, tgt.at[0]),
                (cur_hbm, anc.at[0]),
                (vol_hbm, vol),
                (val_hbm, val.at[0]),
            ]
        )
    ]
    for load in loads:
        load.start()

    barrier = pltpu.get_barrier_semaphore()
    far_first = list(range(g - 1, 0, -1)), list(range(h - 1, 0, -1))
    for masks, offsets in zip((inner, outer), far_first):
        for offset in offsets:
            pl.semaphore_signal(barrier, inc=1, device_id={"blk": me ^ masks[offset]}, device_id_type=MESH)

    def copy(src, dst, send, recv, mask):
        return pltpu.make_async_remote_copy(
            src_ref=src,
            dst_ref=dst,
            send_sem=send,
            recv_sem=recv,
            device_id={"blk": me ^ mask},
            device_id_type=MESH,
        )

    def tgt_sem(q):
        return tgt_recv.at[0 if q < near else 1]

    tgt_copies = {q: copy(tgt.at[0], tgt.at[q], send_sem.at[0], tgt_sem(q), inner[q]) for q in far_first[0]}
    anc_copies = {s: copy(anc.at[0], anc.at[s], send_sem.at[1], anc_recv, outer[s]) for s in far_first[1]}
    val_copies = {q: copy(val.at[0], val.at[q], send_sem.at[2], val_recv, inner[q]) for q in far_first[0]}
    dens_copies = {q: copy(dens_own, dens_in.at[q], send_sem.at[3], dens_recv, inner[q]) for q in far_first[0]}
    part_copies = {s: copy(part_own.at[s], part_in.at[s], send_sem.at[4], part_recv, outer[s]) for s in far_first[1]}

    def several(ref, first, last, send, recv):
        span = ref.at[pl.ds(first, last - first)]
        return copy(span, span, send, recv, 1)

    reading = reader(me, inner)
    pl.semaphore_wait(barrier, (h - 1) + (g - 1))

    @pl.when(reading)
    def _():
        for q in far_first[0]:
            copy(facts_ref, facts, send_sem.at[5], facts_recv, inner[q]).start()
        facts[...] = facts_ref[...]

    loads[0].wait()
    for each in tgt_copies.values():
        each.start()
    loads[1].wait()
    for each in anc_copies.values():
        each.start()
    for load in loads[2:]:
        load.wait()
    for each in val_copies.values():
        each.start()

    if g > 1:

        @pl.when(jnp.logical_not(reading))
        def _():
            copy(facts_ref, facts, send_sem.at[5], facts_recv, 1).wait_recv()

    dates, assets = vol.shape
    date = facts[0:1, 0:1].astype(jnp.int32)
    strike = facts[0:1, 128:129]
    picked = lax.broadcasted_iota(jnp.int32, (dates, assets), 0) == date
    vol_lanes = jnp.sum(jnp.where(picked, vol[...], 0.0), axis=0, keepdims=True)
    eye = lax.broadcasted_iota(jnp.int32, (assets, assets), 0) == lax.broadcasted_iota(
        jnp.int32, (assets, assets), 1
    )
    vol_row = jnp.sum(jnp.where(eye, vol_lanes, 0.0), axis=1, keepdims=True)
    scale = math.sqrt(math.log2(math.e)) / (vol_row * math.sqrt(step_years))
    drift = (rate_year - 0.5 * vol_row * vol_row) * step_years

    def take_anchor(s):
        rows[s] = jnp.transpose(anchor_stack((anc[s] + drift) * scale))

    def take_target(q):
        columns[q] = target_stack(tgt[q] * scale)

    def block(s, q):
        exponent = jnp.dot(rows[s], columns[q], preferred_element_type=jnp.float32)
        weights = jnp.exp2(exponent)
        kmat[s, :, q * n : (q + 1) * n] = weights
        return jnp.sum(weights.reshape(n // 8, 8, n), axis=0)

    density = {}
    take_anchor(0)
    take_target(0)
    density[0] = block(0, 0)
    if near > 1:
        several(tgt, 1, 2, send_sem.at[0], tgt_recv.at[0]).wait_recv()
        take_target(1)
        density[1] = block(0, 1)
    if h > 1:
        several(anc, 1, h, send_sem.at[1], anc_recv).wait_recv()
        for s in range(1, h):
            take_anchor(s)
        for s in range(1, h):
            for q in range(near):
                density[q] = density[q] + block(s, q)
    for q in range(near):
        dens_own[q] = jnp.sum(density[q], axis=0, keepdims=True)
    if g > near:
        several(tgt, near, g, send_sem.at[0], tgt_recv.at[1]).wait_recv()
        for q in range(near, g):
            take_target(q)
        for q in range(near, g):
            density[q] = jnp.zeros((8, n), jnp.float32)
        for s in range(h):
            for q in range(near, g):
                density[q] = density[q] + block(s, q)
        for q in range(near, g):
            dens_own[q] = jnp.sum(density[q], axis=0, keepdims=True)

    for each in dens_copies.values():
        each.start()
    best = jnp.max(jnp.exp(anc[0]), axis=0, keepdims=True)
    payoff = jnp.maximum(best - strike, 0.0)
    if g > 1:
        several(val, 1, g, send_sem.at[2], val_recv).wait_recv()
        several(dens_in, 1, g, send_sem.at[3], dens_recv).wait_recv()
    worth, inverse = {}, {}
    for q in range(g):
        total = dens_own[q]
        for p in range(1, g):
            total = total + dens_in[p, q ^ p]
        inverse[q] = 1.0 / total
        worth[q] = val[q] / total

    for s in [*far_first[1], 0]:
        for r in range(0, n, 128):
            weighted = jnp.zeros((128, 128), jnp.float32)
            mass = jnp.zeros((128, 128), jnp.float32)
            for q in range(g):
                for c in range(0, n, 128):
                    tile = kmat[s, r : r + 128, q * n + c : q * n + c + 128]
                    weighted = weighted + tile * worth[q][:, c : c + 128]
                    mass = mass + tile * inverse[q][:, c : c + 128]
            part_own[s, 0:1, r : r + 128] = jnp.sum(jnp.transpose(weighted), axis=0, keepdims=True)
            part_own[s, 1:2, r : r + 128] = jnp.sum(jnp.transpose(mass), axis=0, keepdims=True)
        if s:
            part_copies[s].start()
    sums = part_own[0]
    if h > 1:
        several(part_in, 1, h, send_sem.at[4], part_recv).wait_recv()
    for s in range(1, h):
        sums = sums + part_in[s]
    weighted_ref[...] = sums[0]
    mass_ref[...] = sums[1]
    payoff_ref[...] = payoff.reshape(n)
    if g > 1:
        several(tgt, 1, g, send_sem.at[0], tgt_recv.at[0]).wait_send()
        several(val, 1, g, send_sem.at[2], val_recv).wait_send()
        several(dens_in, 1, g, send_sem.at[3], dens_recv).wait_send()
    if h > 1:
        several(anc, 1, h, send_sem.at[1], anc_recv).wait_send()
        several(part_in, 1, h, send_sem.at[4], part_recv).wait_send()

    @pl.when(reading)
    def _():
        for q in far_first[0]:
            copy(facts_ref, facts, send_sem.at[5], facts_recv, inner[q]).wait_send()


def body(count, current_states, next_states, next_values, vol_table, date_index, strike):
    assets, n = current_states.shape
    inner, outer = grid_masks(count)
    g, h = len(inner), len(outer)
    f32, bf16 = jnp.float32, jnp.bfloat16
    dma = pltpu.SemaphoreType.DMA
    row = pltpu.VMEM((n,), f32)
    facts = lax.cond(
        reader(lax.axis_index("blk"), inner),
        lambda date, strike: jnp.concatenate([jnp.broadcast_to(date.astype(f32), (128,)), jnp.broadcast_to(strike, (128,))]),
        lambda date, strike: jnp.zeros((256,), f32),
        date_index,
        strike,
    )
    w, m, p = pl.pallas_call(
        functools.partial(kernel, inner, outer),
        out_shape=(row, row, row),
        in_specs=[pl.BlockSpec(memory_space=pltpu.HBM)] * 4 + [pl.BlockSpec(memory_space=pltpu.VMEM)],
        out_specs=(pl.BlockSpec(memory_space=pltpu.VMEM),) * 3,
        scratch_shapes=[
            pltpu.VMEM((h, assets, n), f32),
            pltpu.VMEM((g, assets, n), f32),
            pltpu.VMEM((g, 1, n), f32),
            pltpu.VMEM(vol_table.shape, f32),
            pltpu.VMEM((1, 256), f32),
            pltpu.VMEM((h, n, 8 * assets), bf16),
            pltpu.VMEM((g, 8 * assets, n), bf16),
            pltpu.VMEM((h, n, g * n), f32),
            pltpu.VMEM((g, 1, n), f32),
            pltpu.VMEM((g, g, 1, n), f32),
            pltpu.VMEM((h, 2, n), f32),
            pltpu.VMEM((h, 2, n), f32),
            dma((4,)),
            dma((6,)),
            dma((2,)),
            dma,
            dma,
            dma,
            dma,
            dma,
        ],
        compiler_params=pltpu.CompilerParams(collective_id=0, has_side_effects=True),
    )(current_states, next_states, next_values.reshape(1, n), vol_table, facts.reshape(1, 256))
    c = math.exp(-rate_year * step_years) * w / m
    return (c, jnp.maximum(p, c))


def solution(mesh):
    placed = (
        P(None, ("groups", "blk")),
        P(None, ("groups", "blk")),
        P(("groups", "blk")),
        P(),
        P(),
        P(),
    )
    return jax.shard_map(
        functools.partial(body, mesh.shape["blk"]),
        mesh=mesh,
        in_specs=placed,
        out_specs=(P(("groups", "blk")), P(("groups", "blk"))),
        check_vma=False,
    )
```

```python
import functools
import math

import jax
import jax.numpy as jnp
from jax import lax
from jax.experimental import pallas as pl
from jax.experimental.pallas import tpu as pltpu
from jax.sharding import PartitionSpec as P

rate_year = 0.05
step_years = 0.1
MESH = pl.DeviceIdType.MESH


def grid_masks(count):
    digits = count.bit_length() - 1
    assert 2**digits == count
    inner_digits = digits // 2
    inner_units = ([1] + [1 << (digits - k) for k in range(1, inner_digits)])[:inner_digits]
    outer_units = [1 << k for k in range(digits) if 1 << k not in inner_units]
    if inner_units and outer_units:
        outer_units[-1] |= 1

    def span(units):
        masks = [0]
        for unit in units:
            masks += [mask ^ unit for mask in masks]
        return masks

    return span(inner_units), span(outer_units)


def reader(place, inner):
    digits = functools.reduce(lambda a, b: a | b, inner)
    return (place & digits) == (digits & 1)


def split3(x):
    high = x.astype(jnp.bfloat16)
    rest = x - high.astype(jnp.float32)
    mid = rest.astype(jnp.bfloat16)
    low = (rest - mid.astype(jnp.float32)).astype(jnp.bfloat16)
    return high, mid, low


def norm_rows(x, first):
    norm = -0.5 * jnp.sum(x * x, axis=0, keepdims=True)
    pieces = [piece.astype(jnp.float32) for piece in split3(norm)]
    row = lax.broadcasted_iota(jnp.int32, (16, x.shape[1]), 0)
    at = 0 if first else 3
    rows = jnp.where((row >= 3 - at) & (row < 6 - at), 1.0, 0.0)
    for number, piece in enumerate(pieces):
        rows = jnp.where(row == at + number, piece, rows)
    return rows.astype(jnp.bfloat16)


def anchor_stack(x):
    high, mid, low = split3(x)
    zero = jnp.zeros_like(high)
    return jnp.concatenate([high, high, high, mid, mid, low, norm_rows(x, True), zero], axis=0)


def target_stack(x):
    high, mid, low = split3(x)
    zero = jnp.zeros_like(high)
    return jnp.concatenate([high, mid, low, high, mid, high, norm_rows(x, False), zero], axis=0)


def kernel(
    inner,
    outer,
    cur_hbm,
    next_hbm,
    val_hbm,
    vol_hbm,
    facts_ref,
    weighted_ref,
    mass_ref,
    payoff_ref,
    anc,
    tgt,
    val,
    vol,
    facts,
    rows,
    columns,
    kmat,
    dens_own,
    dens_in,
    part_own,
    part_in,
    in_sem,
    send_sem,
    tgt_recv,
    anc_recv,
    val_recv,
    facts_recv,
    dens_recv,
    part_recv,
):
    g, h = len(inner), len(outer)
    n = anc.shape[2]
    near = min(g, 2)
    me = lax.axis_index("blk")

    loads = [
        pltpu.make_async_copy(src, dst, in_sem.at[number])
        for number, (src, dst) in enumerate(
            [
                (next_hbm, tgt.at[0]),
                (cur_hbm, anc.at[0]),
                (vol_hbm, vol),
                (val_hbm, val.at[0]),
            ]
        )
    ]
    for load in loads:
        load.start()

    barrier = pltpu.get_barrier_semaphore()
    far_first = list(range(g - 1, 0, -1)), list(range(h - 1, 0, -1))
    for masks, offsets in zip((inner, outer), far_first):
        for offset in offsets:
            pl.semaphore_signal(barrier, inc=1, device_id={"blk": me ^ masks[offset]}, device_id_type=MESH)

    def copy(src, dst, send, recv, mask):
        return pltpu.make_async_remote_copy(
            src_ref=src,
            dst_ref=dst,
            send_sem=send,
            recv_sem=recv,
            device_id={"blk": me ^ mask},
            device_id_type=MESH,
        )

    def tgt_sem(q):
        return tgt_recv.at[0 if q < near else 1]

    tgt_copies = {q: copy(tgt.at[0], tgt.at[q], send_sem.at[0], tgt_sem(q), inner[q]) for q in far_first[0]}
    anc_copies = {s: copy(anc.at[0], anc.at[s], send_sem.at[1], anc_recv.at[min(s - 1, 1)], outer[s]) for s in far_first[1]}
    val_copies = {q: copy(val.at[0], val.at[q], send_sem.at[2], val_recv, inner[q]) for q in far_first[0]}
    dens_copies = {q: copy(dens_own, dens_in.at[q], send_sem.at[3], dens_recv, inner[q]) for q in far_first[0]}
    part_copies = {s: copy(part_own.at[s], part_in.at[s], send_sem.at[4], part_recv, outer[s]) for s in far_first[1]}

    def several(ref, first, last, send, recv):
        span = ref.at[pl.ds(first, last - first)]
        return copy(span, span, send, recv, 1)

    reading = reader(me, inner)
    pl.semaphore_wait(barrier, (h - 1) + (g - 1))

    @pl.when(reading)
    def _():
        for q in far_first[0]:
            copy(facts_ref, facts, send_sem.at[5], facts_recv, inner[q]).start()
        facts[...] = facts_ref[...]

    loads[0].wait()
    def send_far(turn):
        for pair in range(near, g, 2):
            q = pair + (me + turn) % 2
            copy(tgt.at[0], tgt.at[q], send_sem.at[0], tgt_recv.at[1], inner[pair] ^ (me + turn) % 2).start()

    send_far(0)
    if near > 1:
        tgt_copies[1].start()
    loads[1].wait()
    for each in anc_copies.values():
        each.start()
    for load in loads[2:]:
        load.wait()
    for each in val_copies.values():
        each.start()
    send_far(1)

    if g > 1:

        @pl.when(jnp.logical_not(reading))
        def _():
            copy(facts_ref, facts, send_sem.at[5], facts_recv, 1).wait_recv()

    dates, assets = vol.shape
    date = facts[0:1, 0:1].astype(jnp.int32)
    strike = facts[0:1, 128:129]
    picked = lax.broadcasted_iota(jnp.int32, (dates, assets), 0) == date
    vol_lanes = jnp.sum(jnp.where(picked, vol[...], 0.0), axis=0, keepdims=True)
    eye = lax.broadcasted_iota(jnp.int32, (assets, assets), 0) == lax.broadcasted_iota(
        jnp.int32, (assets, assets), 1
    )
    vol_row = jnp.sum(jnp.where(eye, vol_lanes, 0.0), axis=1, keepdims=True)
    scale = math.sqrt(math.log2(math.e)) / (vol_row * math.sqrt(step_years))
    drift = (rate_year - 0.5 * vol_row * vol_row) * step_years

    def take_anchor(s):
        rows[s] = jnp.transpose(anchor_stack((anc[s] + drift) * scale))

    def take_target(q):
        columns[q] = target_stack(tgt[q] * scale)

    def block(s, q):
        exponent = jnp.dot(rows[s], columns[q], preferred_element_type=jnp.float32)
        weights = jnp.exp2(exponent)
        kmat[s, :, q * n : (q + 1) * n] = weights
        return jnp.sum(weights.reshape(n // 8, 8, n), axis=0)

    first = min(h, 2)
    take_anchor(0)
    take_target(0)
    if near > 1:
        several(tgt, 1, 2, send_sem.at[0], tgt_recv.at[0]).wait_recv()
        take_target(1)
    density = {q: block(0, q) for q in range(near)}
    if h > 1:
        several(anc, 1, 2, send_sem.at[1], anc_recv.at[0]).wait_recv()
        take_anchor(1)
        for q in range(near):
            density[q] = density[q] + block(1, q)
    if g > near:
        several(tgt, near, g, send_sem.at[0], tgt_recv.at[1]).wait_recv()
    if h > first:
        several(anc, first, h, send_sem.at[1], anc_recv.at[1]).wait_recv()
    for q in range(near, g):
        take_target(q)
        density[q] = jnp.zeros((8, n), jnp.float32)
    for s in range(first, h):
        take_anchor(s)
    for s in range(h):
        for q in range(near if s < first else 0, g):
            density[q] = density[q] + block(s, q)
    for q in range(g):
        dens_own[q] = jnp.sum(density[q], axis=0, keepdims=True)

    for each in dens_copies.values():
        each.start()
    best = jnp.max(jnp.exp(anc[0]), axis=0, keepdims=True)
    payoff = jnp.maximum(best - strike, 0.0)
    if g > 1:
        several(val, 1, g, send_sem.at[2], val_recv).wait_recv()
        several(dens_in, 1, g, send_sem.at[3], dens_recv).wait_recv()
    worth, inverse = {}, {}
    for q in range(g):
        total = dens_own[q]
        for p in range(1, g):
            total = total + dens_in[p, q ^ p]
        inverse[q] = 1.0 / total
        worth[q] = val[q] / total

    for s in [*far_first[1], 0]:
        for r in range(0, n, 128):
            weighted = jnp.zeros((128, 128), jnp.float32)
            mass = jnp.zeros((128, 128), jnp.float32)
            for q in range(g):
                for c in range(0, n, 128):
                    tile = kmat[s, r : r + 128, q * n + c : q * n + c + 128]
                    weighted = weighted + tile * worth[q][:, c : c + 128]
                    mass = mass + tile * inverse[q][:, c : c + 128]
            part_own[s, 0:1, r : r + 128] = jnp.sum(jnp.transpose(weighted), axis=0, keepdims=True)
            part_own[s, 1:2, r : r + 128] = jnp.sum(jnp.transpose(mass), axis=0, keepdims=True)
        if s:
            part_copies[s].start()
    sums = part_own[0]
    if h > 1:
        several(part_in, 1, h, send_sem.at[4], part_recv).wait_recv()
    for s in range(1, h):
        sums = sums + part_in[s]
    weighted_ref[...] = sums[0]
    mass_ref[...] = sums[1]
    payoff_ref[...] = payoff.reshape(n)
    if g > 1:
        several(tgt, 1, g, send_sem.at[0], tgt_recv.at[0]).wait_send()
        several(val, 1, g, send_sem.at[2], val_recv).wait_send()
        several(dens_in, 1, g, send_sem.at[3], dens_recv).wait_send()
    if h > 1:
        several(anc, 1, h, send_sem.at[1], anc_recv.at[0]).wait_send()
        several(part_in, 1, h, send_sem.at[4], part_recv).wait_send()

    @pl.when(reading)
    def _():
        for q in far_first[0]:
            copy(facts_ref, facts, send_sem.at[5], facts_recv, inner[q]).wait_send()


def body(count, current_states, next_states, next_values, vol_table, date_index, strike):
    assets, n = current_states.shape
    inner, outer = grid_masks(count)
    g, h = len(inner), len(outer)
    f32, bf16 = jnp.float32, jnp.bfloat16
    dma = pltpu.SemaphoreType.DMA
    row = pltpu.VMEM((n,), f32)
    facts = lax.cond(
        reader(lax.axis_index("blk"), inner),
        lambda date, strike: jnp.concatenate([jnp.broadcast_to(date.astype(f32), (128,)), jnp.broadcast_to(strike, (128,))]),
        lambda date, strike: jnp.zeros((256,), f32),
        date_index,
        strike,
    )
    w, m, p = pl.pallas_call(
        functools.partial(kernel, inner, outer),
        out_shape=(row, row, row),
        in_specs=[pl.BlockSpec(memory_space=pltpu.HBM)] * 4 + [pl.BlockSpec(memory_space=pltpu.VMEM)],
        out_specs=(pl.BlockSpec(memory_space=pltpu.VMEM),) * 3,
        scratch_shapes=[
            pltpu.VMEM((h, assets, n), f32),
            pltpu.VMEM((g, assets, n), f32),
            pltpu.VMEM((g, 1, n), f32),
            pltpu.VMEM(vol_table.shape, f32),
            pltpu.VMEM((1, 256), f32),
            pltpu.VMEM((h, n, 8 * assets), bf16),
            pltpu.VMEM((g, 8 * assets, n), bf16),
            pltpu.VMEM((h, n, g * n), f32),
            pltpu.VMEM((g, 1, n), f32),
            pltpu.VMEM((g, g, 1, n), f32),
            pltpu.VMEM((h, 2, n), f32),
            pltpu.VMEM((h, 2, n), f32),
            dma((4,)),
            dma((6,)),
            dma((2,)),
            dma((2,)),
            dma,
            dma,
            dma,
            dma,
        ],
        compiler_params=pltpu.CompilerParams(collective_id=0, has_side_effects=True),
    )(current_states, next_states, next_values.reshape(1, n), vol_table, facts.reshape(1, 256))
    c = math.exp(-rate_year * step_years) * w / m
    return (c, jnp.maximum(p, c))


def solution(mesh):
    placed = (
        P(None, ("groups", "blk")),
        P(None, ("groups", "blk")),
        P(("groups", "blk")),
        P(),
        P(),
        P(),
    )
    return jax.shard_map(
        functools.partial(body, mesh.shape["blk"]),
        mesh=mesh,
        in_specs=placed,
        out_specs=(P(("groups", "blk")), P(("groups", "blk"))),
        check_vma=False,
    )
```
